32 devices in a mesh: gx: 8 (over z, x), gy: 4 (over y, core).
Axes of the slice: x: 2, y: 2, z: 4, core: 2. Of those that a mesh axis runs over, the one named last changes fastest.
Arguments:
- state: float32 [65536, 128], P(('gx', 'gy')), may hold values from 0 to 1
- velocity: bfloat16 [3, 3, 128, 64, 128], P(None, None, 'gx', 'gy'), may hold values from -3 to 3
- cells: int32 [3, 3, 65536], P(None, None, ('gx', 'gy')), may hold values from -1 to 126, as said below
- slots: int32 [3, 65536], P(None, ('gx', 'gy')), may hold values from 0 to 2047, as said below
- counts: int32 [3, 8, 4, 8], P(None, 'gx', 'gy'), may hold values from 0 to 64, as said below
Outputs:
- final_state: float32 [65536, 128], P(('gx', 'gy'))
The draws below stay inside these ranges and needn't reach their ends.
Inputs may be any that keep to these rules, and one draw needn't show every extreme that they name: For every section and device the 2048 values of slots are a permutation of 0 to 2047. counts[s, i, j, r] equals counts[s, i', j', r xor 1] where (i', j') is the neighbour of (i, j) in direction r; some device sends exactly 64 in every section. cells[s, 0] lies in -1 to 15, cells[s, 1] in -1 to 15, cells[s, 2] in 0 to 126.
All inputs are finite; a program needn't handle non-finite values.
Results may differ from the reference program's by a relative error of at most 0.0003.
Values may be sent and summed in bfloat16 or wider, within the bound.
A program may use at most 64 MiB of HBM per device.

```python
import jax
import jax.numpy as jnp

CX = 16
CY = 16
NZ = 128
PART_DEV = 2048
CAP = 64
S = 128
SECTIONS = 3
NX = 128
NY = 64
NPART = 65536
N_GX = 8
N_GY = 4


def draw_counts(key, part):
    forward = jax.random.randint(key, (SECTIONS, N_GX, N_GY, 4), CAP // 4, CAP + 1)
    picks = jax.random.randint(jax.random.fold_in(key, 7), (SECTIONS,), 0, N_GX * N_GY)
    hot = (jnp.arange(N_GX * N_GY)[None, :] == picks[:, None]).reshape(SECTIONS, N_GX, N_GY)
    east = jnp.where(hot, CAP, forward[..., 0])
    north = forward[..., 1]
    rising = forward[..., 2]
    falling = forward[..., 3]
    table = jnp.stack([east, jnp.roll(east, 1, axis=1), north, jnp.roll(north, 1, axis=2), rising, jnp.roll(rising, (1, 1), axis=(1, 2)), falling, jnp.roll(falling, (1, -1), axis=(1, 2))], axis=-1)
    return table.astype(jnp.int32)


def draw_slots(key, part):
    scores = jax.random.randint(key, (SECTIONS, N_GX * N_GY, PART_DEV), 0, 2 ** 18)
    scores = scores * PART_DEV + jnp.arange(PART_DEV, dtype=jnp.int32)[None, None, :]
    order = jnp.argsort(scores, axis=-1, stable=True).astype(jnp.int32)
    return order.reshape(SECTIONS, N_GX * N_GY * PART_DEV)


def draw_cells(key, part):
    npart = N_GX * N_GY * PART_DEV
    cell_x = jax.random.randint(jax.random.fold_in(key, 1), (SECTIONS, npart), -1, CX)
    cell_y = jax.random.randint(jax.random.fold_in(key, 2), (SECTIONS, npart), -1, CY)
    cell_z = jax.random.randint(jax.random.fold_in(key, 3), (SECTIONS, npart), 0, NZ - 1)
    return jnp.stack([cell_x, cell_y, cell_z], axis=1).astype(jnp.int32)


def level_of(key, shape, split, low, top_value):
    gain = 1.0
    for position, parts in split:
        draws = jax.random.uniform(jax.random.fold_in(jax.random.fold_in(key, 6), position), (parts,), jnp.float32, low / len(split), top_value / len(split))
        gain = gain * jnp.repeat(jnp.exp(draws), shape[position] // parts).reshape((-1,) + (1,) * (len(shape) - 1 - position))
    return gain


def normal_values(own_key, dims, scale, reach, pieces=(), held_as=jnp.bfloat16):
    gain = level_of(own_key, dims, pieces, -0.22, 0.18) if pieces else 1.0
    array = jax.random.normal(own_key, dims, jnp.float32) * scale * gain
    return jnp.minimum(jnp.maximum(array, -reach), reach).astype(held_as)


def setup_inputs(seed: int = 0) -> dict:
    key_of = jax.random.split(jax.random.key(seed), 6)
    state = jnp.clip(1.0 * jax.random.uniform(key_of[0], (NPART, S), jnp.float32) ** level_of(key_of[0], (NPART, S), ((0, 32),), -0.2, 0.2), 0.0, 1.0)
    velocity = normal_values(key_of[1], (SECTIONS, 3, NX, NY, NZ), 0.4, 3.0, ((2, 8), (3, 4)))
    cells = draw_cells(jax.random.fold_in(key_of[5], 71), 0)
    slots = draw_slots(jax.random.fold_in(key_of[5], 71), 0)
    counts = draw_counts(jax.random.fold_in(key_of[5], 71), 0)
    return dict(state=state, velocity=velocity, cells=cells, slots=slots, counts=counts)


GAMMA = (8.0 / 15.0, 5.0 / 12.0, 3.0 / 4.0)
ZETA = (0.0, -17.0 / 60.0, -5.0 / 12.0)
OFFSETS = ((1, 0), (-1, 0), (0, 1), (0, -1), (1, 1), (-1, -1), (1, -1), (-1, 1))
OPPOSITE = (1, 0, 3, 2, 5, 4, 7, 6)


def reference(state, velocity, cells, slots, counts):
    devices = N_GX * N_GY
    npart = devices * PART_DEV
    owner = jnp.arange(npart, dtype=jnp.int32) // PART_DEV
    row_i = owner // N_GY
    col_j = owner % N_GY
    lanes = jnp.arange(devices, dtype=jnp.int32)
    lane_i = lanes // N_GY
    lane_j = lanes % N_GY
    within = jnp.arange(CAP, dtype=jnp.int32)
    for section in range(SECTIONS):
        field = velocity[section]
        base_x = row_i * CX + cells[section, 0]
        base_y = col_j * CY + cells[section, 1]
        base_z = cells[section, 2]
        frac = state[:, 0:3]
        sampled = jnp.zeros((3, npart), jnp.float32)
        for a in (0, 1):
            for b in (0, 1):
                for c in (0, 1):
                    weight_x = frac[:, 0] if a else 1.0 - frac[:, 0]
                    weight_y = frac[:, 1] if b else 1.0 - frac[:, 1]
                    weight_z = frac[:, 2] if c else 1.0 - frac[:, 2]
                    index_x = (base_x + a) % NX
                    index_y = (base_y + b) % NY
                    values = field[:, index_x, index_y, base_z + c].astype(jnp.float32)
                    sampled = sampled + (weight_x * weight_y * weight_z)[None, :] * values
        speed = sampled.T
        moved = frac + GAMMA[section] * speed + ZETA[section] * state[:, 3:6]
        state = jnp.concatenate([moved, speed, state[:, 6:]], axis=1)
        order = slots[section].reshape(devices, PART_DEV)
        tally = counts[section].reshape(devices, 8)
        source = jnp.arange(npart, dtype=jnp.int32)
        for direction in range(8):
            off_x, off_y = OFFSETS[direction]
            back = OPPOSITE[direction]
            neighbour = ((lane_i + off_x) % N_GX) * N_GY + (lane_j + off_y) % N_GY
            far = neighbour[:, None] * PART_DEV + order[neighbour, back * CAP:(back + 1) * CAP]
            near = lanes[:, None] * PART_DEV + order[:, direction * CAP:(direction + 1) * CAP]
            picked = jnp.where(within[None, :] < tally[:, direction:direction + 1], far, near)
            source = source.at[near.reshape(-1)].set(picked.reshape(-1).astype(jnp.int32))
        state = state[source]
    return state
```

```python
import functools

import jax
import jax.numpy as jnp
from jax import lax
from jax.experimental import pallas as pl
from jax.experimental.pallas import tpu as pltpu
from jax.sharding import PartitionSpec as P

GAMMA = (8.0 / 15.0, 5.0 / 12.0, 3.0 / 4.0)
ZETA = (0.0, -17.0 / 60.0, -5.0 / 12.0)
OFFSETS = ((1, 0), (-1, 0), (0, 1), (0, -1), (1, 1), (-1, -1), (1, -1), (-1, 1))
SPARE = 8
MESH = pl.DeviceIdType.MESH
VMEM = pl.BlockSpec(memory_space=pltpu.VMEM)
SMEM = pl.BlockSpec(memory_space=pltpu.SMEM)


def neighbour(r, sizes):
    off_x, off_y = OFFSETS[r]
    i, j = lax.axis_index("gx"), lax.axis_index("gy")
    return (lax.rem(i + off_x + sizes[0], sizes[0]), lax.rem(j + off_y + sizes[1], sizes[1]))


def greet(sizes):
    barrier = pltpu.get_barrier_semaphore()
    for r in range(8):
        pl.semaphore_signal(barrier, inc=1, device_id=neighbour(r, sizes), device_id_type=MESH)
    pl.semaphore_wait(barrier, 8)


def exchange_all(pairs, send_sem, recv_sem, sizes):
    copies = []
    for r in (4, 5, 6, 7, 0, 1, 2, 3):
        src, dst = pairs[r]
        copy = pltpu.make_async_remote_copy(
            src_ref=src,
            dst_ref=dst,
            send_sem=send_sem.at[r],
            recv_sem=recv_sem.at[r ^ 1],
            device_id=neighbour(r, sizes),
            device_id_type=MESH,
        )
        copy.start()
        copies.append(copy)
    for copy in copies:
        copy.wait()


def halo_spans(cx, cy):
    widths = (cy, cy, cx, cx, cy, cy, cy, cy)
    starts = [sum(widths[:r]) for r in range(8)]
    return widths, starts


def halo_kernel(sizes, v_ref, yface_ref, halo_ref, send_sem, recv_sem):
    cx, cy = v_ref.shape[1], v_ref.shape[2]
    widths, starts = halo_spans(cx, cy)
    greet(sizes)
    pairs = []
    for r in range(8):
        off_x, off_y = OFFSETS[r]
        if off_x:
            src = v_ref.at[:, cx - 1 if off_x > 0 else 0]
        else:
            src = yface_ref.at[1 if off_y > 0 else 0]
        dst = halo_ref.at[:, pl.ds(starts[r ^ 1], widths[r ^ 1]), :]
        pairs.append((src, dst))
    exchange_all(pairs, send_sem, recv_sem, sizes)


def exchange_kernel(sizes, out_ref, in_ref, send_sem, recv_sem):
    cap = out_ref.shape[0] // 8
    greet(sizes)
    pairs = [
        (out_ref.at[pl.ds(r * cap, cap)], in_ref.at[pl.ds((r ^ 1) * cap, cap)]) for r in range(8)
    ]
    exchange_all(pairs, send_sem, recv_sem, sizes)


def scatter_rows(goal_ref, section, incoming_ref, rows_ref):
    def body(step, carry):
        for u in range(16):
            t = step * 16 + u
            rows_ref[pl.ds(goal_ref[section, t], 1), :] = incoming_ref[pl.ds(t, 1), :]
        return carry

    lax.fori_loop(0, incoming_ref.shape[0] // 16, body, 0)


def split(parts):
    whole = jnp.concatenate(parts, axis=0)
    high = whole.astype(jnp.bfloat16)
    return high, (whole - high.astype(jnp.float32)).astype(jnp.bfloat16)


def cell_weights(size, cell, frac):
    spots = lax.broadcasted_iota(jnp.int32, (size, cell.shape[1]), 0)
    low, high = 1.0 - frac, frac
    inside = jnp.where(spots == cell, low, 0.0) + jnp.where(spots == cell + 1, high, 0.0)
    return inside, jnp.where(cell == -1, low, 0.0), jnp.where(cell == size - 1, high, 0.0)


def section_kernel(section, dims, *refs):
    if section:
        goal_ref, order_ref, cells_ref, v_ref, halo_ref, state_ref, incoming_ref, rows_ref, leave_ref, plane_ref = refs
    else:
        order_ref, cells_ref, v_ref, halo_ref, state_ref, rows_ref, leave_ref, plane_ref = refs
    cx, cy = dims
    depth = v_ref.shape[2]
    count = cells_ref.shape[2]
    inner = cx * cy
    if section:
        rows_ref[...] = state_ref[...]
        scatter_rows(goal_ref, section - 1, incoming_ref, rows_ref)
        source_ref = rows_ref
    else:
        source_ref = state_ref
    for k in range(3):
        plane_ref[pl.ds(k * depth, depth), 0:inner] = v_ref[3 * section + k].T
        plane_ref[pl.ds(k * depth, depth), inner:] = halo_ref[3 * section + k].T
    block = 256
    for b in range(count // block):
        span = slice(b * block, (b + 1) * block)
        tiles = [source_ref[b * block + h * 128 : b * block + (h + 1) * 128, :] for h in range(block // 128)]
        head = jnp.concatenate([tile.T[0:8] for tile in tiles], axis=1)
        cell = cells_ref[section, :, span]
        wx, wx_low, wx_high = cell_weights(cx, cell[0:1], head[0:1])
        wy, wy_low, wy_high = cell_weights(cy, cell[1:2], head[1:2])
        wz, _, _ = cell_weights(depth, cell[2:3], head[2:3])
        rows_y = lax.broadcasted_iota(jnp.int32, (cy, block), 0)
        parts = [wx[x : x + 1] * wy for x in range(cx)]
        parts += [wx_high * wy, wx_low * wy, wx * wy_high, wx * wy_low]
        parts += [
            jnp.where(rows_y == 0, wx_high * wy_high, 0.0),
            jnp.where(rows_y == cy - 1, wx_low * wy_low, 0.0),
            jnp.where(rows_y == cy - 1, wx_high * wy_low, 0.0),
            jnp.where(rows_y == 0, wx_low * wy_high, 0.0),
        ]
        high, low = split(parts)
        columns = jnp.dot(plane_ref[...], high, preferred_element_type=jnp.float32)
        columns = columns + jnp.dot(plane_ref[...], low, preferred_element_type=jnp.float32)
        speed = jnp.concatenate(
            [
                jnp.sum(columns[k * depth : (k + 1) * depth] * wz, axis=0, keepdims=True)
                for k in range(3)
            ],
            axis=0,
        )
        moved = head[0:3] + GAMMA[section] * speed + ZETA[section] * head[3:6]
        fresh = jnp.concatenate([moved, speed, jnp.zeros((122, block), jnp.float32)], axis=0)
        lanes = lax.broadcasted_iota(jnp.int32, (128, tiles[0].shape[1]), 1)
        for h in range(block // 128):
            turned = fresh[:, h * 128 : (h + 1) * 128].T
            rows_ref[b * block + h * 128 : b * block + (h + 1) * 128, :] = jnp.where(lanes < 6, turned, tiles[h])

    def body(step, carry):
        for u in range(16):
            t = step * 16 + u
            leave_ref[pl.ds(t, 1), :] = rows_ref[pl.ds(order_ref[section, t], 1), :]
        return carry

    lax.fori_loop(0, leave_ref.shape[0] // 16, body, 0)


def last_kernel(section, goal_ref, state_ref, incoming_ref, out_ref, rows_ref):
    rows_ref[...] = state_ref[...]
    scatter_rows(goal_ref, section, incoming_ref, rows_ref)
    out_ref[...] = rows_ref[0 : out_ref.shape[0], :]


def local(sizes, cap, state, velocity, cells, slots, counts):
    sections, _, cx, cy, depth = velocity.shape
    count, width = state.shape
    moving = 8 * cap
    inner = cx * cy
    widths, _ = halo_spans(cx, cy)
    outer = sum(widths)
    field = velocity.reshape(sections * 3, cx, cy, depth)
    yface = jnp.stack([field[:, :, 0, :], field[:, :, cy - 1, :]])
    order = slots[:, 0:moving]
    limits = jnp.repeat(counts.reshape(sections, 8), cap, axis=1)
    within = jnp.tile(jnp.arange(cap, dtype=jnp.int32), 8)[None, :]
    goal = jnp.where(within < limits, order, count)

    def talk(kernel, ident, shape, dtype, *args):
        return pl.pallas_call(
            functools.partial(kernel, sizes),
            out_shape=jax.ShapeDtypeStruct(shape, dtype),
            in_specs=[VMEM] * len(args),
            out_specs=VMEM,
            scratch_shapes=[pltpu.SemaphoreType.DMA((8,)), pltpu.SemaphoreType.DMA((8,))],
            compiler_params=pltpu.CompilerParams(collective_id=ident, has_side_effects=True),
        )(*args)

    halo = talk(halo_kernel, 0, (sections * 3, outer, depth), field.dtype, field, yface)
    flat = field.reshape(sections * 3, inner, depth)
    rows = state
    for section in range(sections):
        specs = [SMEM, VMEM, VMEM, VMEM, VMEM]
        args = [order, cells, flat, halo, rows]
        if section:
            specs = [SMEM] + specs + [VMEM]
            args = [goal] + args + [incoming]
        rows, leaving = pl.pallas_call(
            functools.partial(section_kernel, section, (cx, cy)),
            out_shape=(
                jax.ShapeDtypeStruct((count + SPARE, width), jnp.float32),
                jax.ShapeDtypeStruct((moving, width), jnp.float32),
            ),
            in_specs=specs,
            out_specs=(VMEM, VMEM),
            scratch_shapes=[pltpu.VMEM((3 * depth, inner + outer), jnp.bfloat16)],
        )(*args)
        incoming = talk(exchange_kernel, 1, (moving, width), jnp.float32, leaving)
    return pl.pallas_call(
        functools.partial(last_kernel, sections - 1),
        out_shape=jax.ShapeDtypeStruct((count, width), jnp.float32),
        in_specs=[SMEM, VMEM, VMEM],
        out_specs=VMEM,
        scratch_shapes=[pltpu.VMEM((count + SPARE, width), jnp.float32)],
    )(goal, rows, incoming)


def solution(mesh):
    return jax.shard_map(
        functools.partial(local, (mesh.shape["gx"], mesh.shape["gy"]), 64),
        mesh=mesh,
        in_specs=(
            P(("gx", "gy"), None),
            P(None, None, "gx", "gy", None),
            P(None, None, ("gx", "gy")),
            P(None, ("gx", "gy")),
            P(None, "gx", "gy", None),
        ),
        out_specs=P(("gx", "gy"), None),
        check_vma=False,
    )
```

```python
import functools

import jax
import jax.numpy as jnp
from jax import lax
from jax.experimental import pallas as pl
from jax.experimental.pallas import tpu as pltpu
from jax.sharding import PartitionSpec as P

GAMMA = (8.0 / 15.0, 5.0 / 12.0, 3.0 / 4.0)
ZETA = (0.0, -17.0 / 60.0, -5.0 / 12.0)
OFFSETS = ((1, 0), (-1, 0), (0, 1), (0, -1), (1, 1), (-1, -1), (1, -1), (-1, 1))
SPARE = 8
MESH = pl.DeviceIdType.MESH
VMEM = pl.BlockSpec(memory_space=pltpu.VMEM)
SMEM = pl.BlockSpec(memory_space=pltpu.SMEM)


def neighbour(r, sizes):
    off_x, off_y = OFFSETS[r]
    i, j = lax.axis_index("gx"), lax.axis_index("gy")
    return (lax.rem(i + off_x + sizes[0], sizes[0]), lax.rem(j + off_y + sizes[1], sizes[1]))


def greet(sizes):
    barrier = pltpu.get_barrier_semaphore()
    for r in range(8):
        pl.semaphore_signal(barrier, inc=1, device_id=neighbour(r, sizes), device_id_type=MESH)
    pl.semaphore_wait(barrier, 8)


def send(r, src, dst, sems, group, sizes):
    copy = pltpu.make_async_remote_copy(
        src_ref=src,
        dst_ref=dst,
        send_sem=sems[0].at[group, r],
        recv_sem=sems[1].at[group, r ^ 1],
        device_id=neighbour(r, sizes),
        device_id_type=MESH,
    )
    copy.start()
    return copy


def parts_of(x):
    high = x.astype(jnp.bfloat16)
    rest = x - high.astype(jnp.float32)
    middle = rest.astype(jnp.bfloat16)
    low = (rest - middle.astype(jnp.float32)).astype(jnp.bfloat16)
    return high, middle, low


def cell_weights(size, cell, frac):
    spots = lax.broadcasted_iota(jnp.int32, (size, cell.shape[1]), 0)
    low, high = 1.0 - frac, frac
    inside = jnp.where(spots == cell, low, 0.0) + jnp.where(spots == cell + 1, high, 0.0)
    return inside, jnp.where(cell == -1, low, 0.0), jnp.where(cell == size - 1, high, 0.0)


def gather_rows(order_ref, section, source_ref, leave_ref, cap):
    def body(step, carry):
        for u in range(16):
            t = step * 16 + u
            leave_ref[section, pl.ds(t, 1), :] = source_ref[pl.ds(order_ref[section, t], 1), :]
        return carry

    lax.fori_loop(0, 8 * cap // 16, body, 0)


def build_onehot(slot_ref, section, onehot_ref):
    slot = slot_ref[section]
    moving = slot.shape[1]
    step_rows = 256

    def body(step, carry):
        base = pl.multiple_of(step * step_rows, step_rows)
        spots = lax.broadcasted_iota(jnp.int32, (step_rows, moving), 0) + base
        onehot_ref[pl.ds(base, step_rows), :] = jnp.where(spots == slot, 1.0, 0.0).astype(jnp.bfloat16)
        return carry

    lax.fori_loop(0, onehot_ref.shape[0] // step_rows, body, 0)


def build_plane(section, dims, v_ref, halo_ref, corner_ref, plane_ref):
    cx, cy = dims
    inner = cx * cy
    depth = v_ref.shape[3]
    for k in range(3):
        row = 3 * section + k
        own = v_ref[row].reshape(inner, depth)
        plane_ref[pl.ds(k * depth, depth), 0:inner] = own.T
        faces = halo_ref[row].astype(jnp.float32)
        corners = [corner_ref[d, row : row + 1, :] for d in range(4)]
        filler = jnp.zeros((128 - faces.shape[0] - 4, depth), jnp.float32)
        edge = jnp.concatenate([faces] + corners + [filler], axis=0)
        width = plane_ref.shape[1] - inner
        plane_ref[pl.ds(k * depth, depth), inner:] = edge.T[:, 0:width].astype(jnp.bfloat16)


def sample(section, dims, cells_ref, head_ref, plane_ref):
    cx, cy = dims
    depth = plane_ref.shape[0] // 3
    block = 256

    def body(step, carry):
        span = pl.ds(pl.multiple_of(step * block, block), block)
        head = head_ref[:, span]
        cell = cells_ref[section, :, span]
        wx, wx_low, wx_high = cell_weights(cx, cell[0:1], head[0:1])
        wy, wy_low, wy_high = cell_weights(cy, cell[1:2], head[1:2])
        wz, _, _ = cell_weights(depth, cell[2:3], head[2:3])
        parts = [wx[x : x + 1] * wy for x in range(cx)]
        parts += [wx_high * wy, wx_low * wy, wx * wy_high, wx * wy_low]
        parts += [wx_high * wy_high, wx_low * wy_low, wx_high * wy_low, wx_low * wy_high]
        parts += [jnp.zeros((12, block), jnp.float32)]
        whole = jnp.concatenate(parts, axis=0)
        high = whole.astype(jnp.bfloat16)
        low = (whole - high.astype(jnp.float32)).astype(jnp.bfloat16)
        columns = jnp.dot(plane_ref[...], high, preferred_element_type=jnp.float32)
        columns = columns + jnp.dot(plane_ref[...], low, preferred_element_type=jnp.float32)
        speed = jnp.concatenate(
            [
                jnp.sum(columns[k * depth : (k + 1) * depth] * wz, axis=0, keepdims=True)
                for k in range(3)
            ],
            axis=0,
        )
        moved = head[0:3] + GAMMA[section] * speed + ZETA[section] * head[3:6]
        head_ref[:, span] = jnp.concatenate([moved, speed, jnp.ones((2, block), jnp.float32)], axis=0)
        return carry

    lax.fori_loop(0, head_ref.shape[1] // block, body, 0)


def steps_kernel(
    sizes,
    cap,
    order_ref,
    slot_ref,
    taken_ref,
    cells_ref,
    v_ref,
    yface_ref,
    away_ref,
    state_ref,
    head_ref,
    arrived_ref,
    rows_ref,
    leave_ref,
    onehot_ref,
    plane_ref,
    halo_ref,
    corner_ref,
    head_out_ref,
    head_in_ref,
    send_sem,
    recv_sem,
):
    sems = (send_sem, recv_sem)
    sections = slot_ref.shape[0]
    cx, cy = v_ref.shape[1], v_ref.shape[2]
    count = state_ref.shape[0]
    moving = 8 * cap
    starts = (0, cy, 2 * cy, 2 * cy + cx)
    widths = (cy, cy, cx, cx)
    greet(sizes)

    halos = []
    for section in range(sections):
        group = []
        fields = pl.ds(3 * section, 3)
        for r in range(4):
            off_x, off_y = OFFSETS[r]
            src = v_ref.at[fields, cx - 1 if off_x > 0 else 0] if off_x else yface_ref.at[r - 2, fields]
            dst = halo_ref.at[fields, pl.ds(starts[r ^ 1], widths[r ^ 1]), :]
            group.append(send(r, src, dst, sems, section, sizes))
        if section == 0:
            for r in range(4, 8):
                group.append(send(r, away_ref.at[r - 4], corner_ref.at[(r ^ 1) - 4], sems, section, sizes))
        halos.append(group)

    def send_rows(section):
        gather_rows(order_ref, section, rows_ref, leave_ref, cap)
        return [
            send(
                r,
                leave_ref.at[section, pl.ds(r * cap, cap)],
                arrived_ref.at[pl.ds(section * moving + (r ^ 1) * cap, cap)],
                sems,
                sections + section,
                sizes,
            )
            for r in range(8)
        ]

    rows_ref[0:count, :] = state_ref[...]
    carried = send_rows(0)
    for b in range(count // 128):
        head_ref[:, b * 128 : (b + 1) * 128] = state_ref[b * 128 : (b + 1) * 128, :].T[0:8]
    for section in range(sections):
        if section == 0:
            build_onehot(slot_ref, 0, onehot_ref.at[0])
        for copy in halos[section]:
            copy.wait()
        build_plane(section, (cx, cy), v_ref, halo_ref, corner_ref, plane_ref)
        sample(section, (cx, cy), cells_ref, head_ref, plane_ref)
        hot = onehot_ref.at[section % 2]
        stacked = jnp.concatenate([part.astype(jnp.float32) for part in parts_of(head_ref[...])], axis=0)
        picked = jnp.dot(stacked.astype(jnp.bfloat16), hot[...], preferred_element_type=jnp.float32)
        leaving = picked[0:8] + picked[8:16] + picked[16:24]
        heads = []
        for r in range(8):
            head_out_ref[section, r] = leaving[:, r * cap : (r + 1) * cap]
        for r in range(8):
            heads.append(
                send(
                    r,
                    head_out_ref.at[section, r],
                    head_in_ref.at[section, r ^ 1],
                    sems,
                    2 * sections + section,
                    sizes,
                )
            )
        for copy in carried:
            copy.wait()
        if section + 1 < sections:
            low = section * moving
            rows_ref[count + low : count + low + moving, :] = arrived_ref[low : low + moving, :]
            carried = send_rows(section + 1)
            build_onehot(slot_ref, section + 1, onehot_ref.at[(section + 1) % 2])
        for copy in heads:
            copy.wait()
        came = jnp.concatenate([head_in_ref[section, r] for r in range(8)], axis=1)
        came = came * taken_ref[section]
        stacked = jnp.concatenate([part.astype(jnp.float32) for part in parts_of(came)], axis=0)
        spread = lax.dot_general(
            stacked.astype(jnp.bfloat16), hot[...], (((1,), (1,)), ((), ())), preferred_element_type=jnp.float32
        )
        placed = spread[0:8] + spread[8:16] + spread[16:24]
        head_ref[...] = jnp.where(placed[6:7] > 0.5, placed, head_ref[...])


def last_kernel(goal_ref, state_ref, arrived_ref, head_ref, out_ref, rows_ref):
    count, width = out_ref.shape
    sections, moving = goal_ref.shape
    rows_ref[0:count, :] = state_ref[...]
    for section in range(sections):

        def body(step, carry):
            for u in range(16):
                t = step * 16 + u
                rows_ref[pl.ds(goal_ref[section, t], 1), :] = arrived_ref[pl.ds(section * moving + t, 1), :]
            return carry

        lax.fori_loop(0, moving // 16, body, 0)
    lanes = lax.broadcasted_iota(jnp.int32, (128, width), 1)
    for b in range(count // 128):
        span = slice(b * 128, (b + 1) * 128)
        full = jnp.concatenate([head_ref[:, span], jnp.zeros((width - 8, 128), jnp.float32)], axis=0)
        out_ref[span, :] = jnp.where(lanes < 6, full.T, rows_ref[span, :])


def local(sizes, cap, state, velocity, cells, slots, counts):
    sections, _, cx, cy, depth = velocity.shape
    count, width = state.shape
    moving = 8 * cap
    fields = sections * 3
    field = velocity.reshape(fields, cx, cy, depth)
    yface = jnp.stack([field[:, :, cy - 1, :], field[:, :, 0, :]])
    away = jnp.stack(
        [field[:, cx - 1, cy - 1], field[:, 0, 0], field[:, cx - 1, 0], field[:, 0, cy - 1]]
    ).astype(jnp.float32)
    away = jnp.pad(away, ((0, 0), (0, -fields % 8), (0, 0)))
    order = slots[:, 0:moving]
    limits = jnp.repeat(counts.reshape(sections, 8), cap, axis=1)
    within = jnp.tile(jnp.arange(cap, dtype=jnp.int32), 8)[None, :]
    taken = within < limits
    goal = jnp.where(taken, order, count)
    places = jnp.arange(moving, dtype=jnp.int32)[:, None]
    sources = [order[0]]
    for section in range(1, sections):
        found = jnp.full((moving,), -1, jnp.int32)
        for past in range(section):
            match = goal[past][:, None] == order[section][None, :]
            found = jnp.maximum(
                found, jnp.max(jnp.where(match, count + past * moving + places, -1), axis=0)
            )
        sources.append(jnp.where(found >= 0, found, order[section]))
    sources = jnp.stack(sources)

    head, arrived = pl.pallas_call(
        functools.partial(steps_kernel, sizes, cap),
        out_shape=(
            jax.ShapeDtypeStruct((8, count), jnp.float32),
            jax.ShapeDtypeStruct((sections * moving, width), jnp.float32),
        ),
        in_specs=[SMEM] + [VMEM] * 7,
        out_specs=(VMEM, VMEM),
        scratch_shapes=[
            pltpu.VMEM((count + (sections - 1) * moving, width), jnp.float32),
            pltpu.VMEM((sections, moving, width), jnp.float32),
            pltpu.VMEM((2, count, moving), jnp.bfloat16),
            pltpu.VMEM((3 * depth, cx * cy + 2 * cx + 2 * cy + 16), jnp.bfloat16),
            pltpu.VMEM((fields, 2 * cx + 2 * cy, depth), jnp.bfloat16),
            pltpu.VMEM(away.shape, jnp.float32),
            pltpu.VMEM((sections, 8, 8, cap), jnp.float32),
            pltpu.VMEM((sections, 8, 8, cap), jnp.float32),
            pltpu.SemaphoreType.DMA((3 * sections, 8)),
            pltpu.SemaphoreType.DMA((3 * sections, 8)),
        ],
        compiler_params=pltpu.CompilerParams(collective_id=0, has_side_effects=True),
    )(
        sources,
        order.reshape(sections, 1, moving),
        taken.astype(jnp.float32).reshape(sections, 1, moving),
        cells,
        field,
        yface,
        away,
        state,
    )
    return pl.pallas_call(
        last_kernel,
        out_shape=jax.ShapeDtypeStruct((count, width), jnp.float32),
        in_specs=[SMEM, VMEM, VMEM, VMEM],
        out_specs=VMEM,
        scratch_shapes=[pltpu.VMEM((count + SPARE, width), jnp.float32)],
    )(goal, state, arrived, head)


def solution(mesh):
    return jax.shard_map(
        functools.partial(local, (mesh.shape["gx"], mesh.shape["gy"]), 64),
        mesh=mesh,
        in_specs=(
            P(("gx", "gy"), None),
            P(None, None, "gx", "gy", None),
            P(None, None, ("gx", "gy")),
            P(None, ("gx", "gy")),
            P(None, "gx", "gy", None),
        ),
        out_specs=P(("gx", "gy"), None),
        check_vma=False,
    )
```

```python
import functools

import jax
import jax.numpy as jnp
from jax import lax
from jax.experimental import pallas as pl
from jax.experimental.pallas import tpu as pltpu
from jax.sharding import PartitionSpec as P

GAMMA = (8.0 / 15.0, 5.0 / 12.0, 3.0 / 4.0)
ZETA = (0.0, -17.0 / 60.0, -5.0 / 12.0)
OFFSETS = ((1, 0), (-1, 0), (0, 1), (0, -1), (1, 1), (-1, -1), (1, -1), (-1, 1))
SPARE = 8
MESH = pl.DeviceIdType.MESH
VMEM = pl.BlockSpec(memory_space=pltpu.VMEM)
SMEM = pl.BlockSpec(memory_space=pltpu.SMEM)


def neighbour(r, sizes):
    off_x, off_y = OFFSETS[r]
    i, j = lax.axis_index("gx"), lax.axis_index("gy")
    return (lax.rem(i + off_x + sizes[0], sizes[0]), lax.rem(j + off_y + sizes[1], sizes[1]))


def greet(sizes):
    barrier = pltpu.get_barrier_semaphore()
    for r in range(8):
        pl.semaphore_signal(barrier, inc=1, device_id=neighbour(r, sizes), device_id_type=MESH)
    pl.semaphore_wait(barrier, 8)


def send(r, src, dst, sems, group, sizes):
    copy = pltpu.make_async_remote_copy(
        src_ref=src,
        dst_ref=dst,
        send_sem=sems[0].at[group, r],
        recv_sem=sems[1].at[group, r ^ 1],
        device_id=neighbour(r, sizes),
        device_id_type=MESH,
    )
    copy.start()
    return copy


def parts_of(x):
    high = x.astype(jnp.bfloat16)
    rest = x - high.astype(jnp.float32)
    middle = rest.astype(jnp.bfloat16)
    low = (rest - middle.astype(jnp.float32)).astype(jnp.bfloat16)
    return high, middle, low


def cell_weights(size, cell, frac):
    spots = lax.broadcasted_iota(jnp.int32, (size, cell.shape[1]), 0)
    low, high = 1.0 - frac, frac
    inside = jnp.where(spots == cell, low, 0.0) + jnp.where(spots == cell + 1, high, 0.0)
    return inside, jnp.where(cell == -1, low, 0.0), jnp.where(cell == size - 1, high, 0.0)


def gather_rows(order_ref, section, source_ref, leave_ref, cap):
    first = section * 8 * cap

    def body(step, carry):
        for u in range(16):
            t = step * 16 + u
            leave_ref[section, pl.ds(t, 1), :] = source_ref[pl.ds(order_ref[first + t], 1), :]
        return carry

    lax.fori_loop(0, 8 * cap // 16, body, 0)


def build_onehot(slot_ref, section, onehot_ref):
    slot = slot_ref[section]
    moving = slot.shape[1]
    step_rows = 256

    def body(step, carry):
        base = pl.multiple_of(step * step_rows, step_rows)
        spots = lax.broadcasted_iota(jnp.int32, (step_rows, moving), 0) + base
        onehot_ref[pl.ds(base, step_rows), :] = jnp.where(spots == slot, 1.0, 0.0).astype(jnp.bfloat16)
        return carry

    lax.fori_loop(0, onehot_ref.shape[0] // step_rows, body, 0)


def build_plane(section, dims, v_ref, halo_ref, corner_ref, plane_ref):
    cx, cy = dims
    inner = cx * cy
    depth = v_ref.shape[3]
    for k in range(3):
        row = 3 * section + k
        own = v_ref[row].reshape(inner, depth)
        plane_ref[pl.ds(k * depth, depth), 0:inner] = own.T
        faces = halo_ref[row].astype(jnp.float32)
        corners = [corner_ref[d, row : row + 1, :] for d in range(4)]
        filler = jnp.zeros((128 - faces.shape[0] - 4, depth), jnp.float32)
        edge = jnp.concatenate([faces] + corners + [filler], axis=0)
        width = plane_ref.shape[1] - inner
        plane_ref[pl.ds(k * depth, depth), inner:] = edge.T[:, 0:width].astype(jnp.bfloat16)


def sample(section, dims, cells_ref, head_ref, plane_ref):
    cx, cy = dims
    depth = plane_ref.shape[0] // 3
    block = 256

    def body(step, carry):
        span = pl.ds(pl.multiple_of(step * block, block), block)
        head = head_ref[:, span]
        cell = cells_ref[section, :, span]
        wx, wx_low, wx_high = cell_weights(cx, cell[0:1], head[0:1])
        wy, wy_low, wy_high = cell_weights(cy, cell[1:2], head[1:2])
        wz, _, _ = cell_weights(depth, cell[2:3], head[2:3])
        parts = [wx[x : x + 1] * wy for x in range(cx)]
        parts += [wx_high * wy, wx_low * wy, wx * wy_high, wx * wy_low]
        parts += [wx_high * wy_high, wx_low * wy_low, wx_high * wy_low, wx_low * wy_high]
        parts += [jnp.zeros((12, block), jnp.float32)]
        whole = jnp.concatenate(parts, axis=0)
        high = whole.astype(jnp.bfloat16)
        low = (whole - high.astype(jnp.float32)).astype(jnp.bfloat16)
        columns = jnp.dot(plane_ref[...], high, preferred_element_type=jnp.float32)
        columns = columns + jnp.dot(plane_ref[...], low, preferred_element_type=jnp.float32)
        speed = jnp.concatenate(
            [
                jnp.sum(columns[k * depth : (k + 1) * depth] * wz, axis=0, keepdims=True)
                for k in range(3)
            ],
            axis=0,
        )
        moved = head[0:3] + GAMMA[section] * speed + ZETA[section] * head[3:6]
        head_ref[:, span] = jnp.concatenate([moved, speed, jnp.ones((2, block), jnp.float32)], axis=0)
        return carry

    lax.fori_loop(0, head_ref.shape[1] // block, body, 0)


def plan_kernel(cap, slots_ref, counts_ref, v_ref, index_ref, slot_ref, taken_ref, yface_ref, away_ref):
    sections, count = slots_ref.shape
    moving = 8 * cap
    fields, inner, depth = v_ref.shape
    cx = yface_ref.shape[2]
    cy = inner // cx
    lanes = lax.broadcasted_iota(jnp.int32, (1, moving), 1)
    within = lax.rem(lanes, cap)
    places = lax.broadcasted_iota(jnp.int32, (moving, moving), 0) + count
    chunks = moving // 128
    columns = []
    for section in range(sections):
        slot = slots_ref[section : section + 1, 0:moving]
        limit = jnp.zeros((1, moving), jnp.int32)
        for r in range(8):
            limit = jnp.where(lanes >= r * cap, counts_ref[section, r], limit)
        taken = within < limit
        goal = jnp.where(taken, slot, count)
        found = jnp.full((1, moving), -1, jnp.int32)
        for past in range(section):
            match = columns[past] == slot
            best = jnp.max(jnp.where(match, places, -1), axis=0, keepdims=True)
            found = jnp.where(best >= 0, best + past * moving, found)
        source = jnp.where(found >= 0, found, slot)
        if section + 1 < sections:
            wide = jnp.broadcast_to(goal.astype(jnp.float32), (8, moving))
            columns.append(wide.T[:, 0:1].astype(jnp.int32))
        slot_ref[section] = slot
        taken_ref[section] = jnp.where(taken, 1.0, 0.0)
        for c in range(chunks):
            span = slice(c * 128, (c + 1) * 128)
            row = section * chunks + c
            index_ref[row : row + 1, :] = source[:, span]
            row += sections * chunks
            index_ref[row : row + 1, :] = goal[:, span]
    row = lax.broadcasted_iota(jnp.int32, (2 * cx + 8, inner), 0)
    place = lax.broadcasted_iota(jnp.int32, (2 * cx + 8, inner), 1)
    want = jnp.where(row < cx, row * cy + cy - 1, (row - cx) * cy)
    for d, spot in enumerate((inner - 1, 0, (cx - 1) * cy, cy - 1)):
        want = jnp.where(row == 2 * cx + d, spot, want)
    pick = jnp.where(want == place, 1.0, 0.0).astype(jnp.bfloat16)
    for f in range(fields):
        edge = jnp.dot(pick, v_ref[f], preferred_element_type=jnp.float32)
        yface_ref[0, f] = edge[0:cx].astype(jnp.bfloat16)
        yface_ref[1, f] = edge[cx : 2 * cx].astype(jnp.bfloat16)
        for d in range(4):
            away_ref[d, f : f + 1, :] = edge[2 * cx + d : 2 * cx + d + 1]


def steps_kernel(
    sizes,
    cap,
    order_ref,
    slot_ref,
    taken_ref,
    cells_ref,
    v_ref,
    yface_ref,
    away_ref,
    state_ref,
    head_ref,
    arrived_ref,
    rows_ref,
    leave_ref,
    onehot_ref,
    plane_ref,
    halo_ref,
    corner_ref,
    head_out_ref,
    head_in_ref,
    send_sem,
    recv_sem,
):
    sems = (send_sem, recv_sem)
    sections = slot_ref.shape[0]
    cx, cy = v_ref.shape[1], v_ref.shape[2]
    count = state_ref.shape[0]
    moving = 8 * cap
    starts = (0, cy, 2 * cy, 2 * cy + cx)
    widths = (cy, cy, cx, cx)
    greet(sizes)

    halos = []
    for section in range(sections):
        group = []
        fields = pl.ds(3 * section, 3)
        for r in range(4):
            off_x, off_y = OFFSETS[r]
            src = v_ref.at[fields, cx - 1 if off_x > 0 else 0] if off_x else yface_ref.at[r - 2, fields]
            dst = halo_ref.at[fields, pl.ds(starts[r ^ 1], widths[r ^ 1]), :]
            group.append(send(r, src, dst, sems, section, sizes))
        if section == 0:
            for r in range(4, 8):
                group.append(send(r, away_ref.at[r - 4], corner_ref.at[(r ^ 1) - 4], sems, section, sizes))
        halos.append(group)

    def send_rows(section):
        gather_rows(order_ref, section, rows_ref, leave_ref, cap)
        return [
            send(
                r,
                leave_ref.at[section, pl.ds(r * cap, cap)],
                arrived_ref.at[pl.ds(section * moving + (r ^ 1) * cap, cap)],
                sems,
                sections + section,
                sizes,
            )
            for r in range(8)
        ]

    rows_ref[0:count, :] = state_ref[...]
    carried = send_rows(0)
    for b in range(count // 128):
        head_ref[:, b * 128 : (b + 1) * 128] = state_ref[b * 128 : (b + 1) * 128, :].T[0:8]
    for section in range(sections):
        if section == 0:
            build_onehot(slot_ref, 0, onehot_ref.at[0])
        for copy in halos[section]:
            copy.wait()
        build_plane(section, (cx, cy), v_ref, halo_ref, corner_ref, plane_ref)
        sample(section, (cx, cy), cells_ref, head_ref, plane_ref)
        hot = onehot_ref.at[section % 2]
        stacked = jnp.concatenate([part.astype(jnp.float32) for part in parts_of(head_ref[...])], axis=0)
        picked = jnp.dot(stacked.astype(jnp.bfloat16), hot[...], preferred_element_type=jnp.float32)
        leaving = picked[0:8] + picked[8:16] + picked[16:24]
        heads = []
        for r in range(8):
            head_out_ref[section, r] = leaving[:, r * cap : (r + 1) * cap]
        for r in range(8):
            heads.append(
                send(
                    r,
                    head_out_ref.at[section, r],
                    head_in_ref.at[section, r ^ 1],
                    sems,
                    2 * sections + section,
                    sizes,
                )
            )
        for copy in carried:
            copy.wait()
        if section + 1 < sections:
            low = section * moving
            rows_ref[count + low : count + low + moving, :] = arrived_ref[low : low + moving, :]
            carried = send_rows(section + 1)
            build_onehot(slot_ref, section + 1, onehot_ref.at[(section + 1) % 2])
        for copy in heads:
            copy.wait()
        came = jnp.concatenate([head_in_ref[section, r] for r in range(8)], axis=1)
        came = came * taken_ref[section]
        stacked = jnp.concatenate([part.astype(jnp.float32) for part in parts_of(came)], axis=0)
        spread = lax.dot_general(
            stacked.astype(jnp.bfloat16), hot[...], (((1,), (1,)), ((), ())), preferred_element_type=jnp.float32
        )
        placed = spread[0:8] + spread[8:16] + spread[16:24]
        head_ref[...] = jnp.where(placed[6:7] > 0.5, placed, head_ref[...])


def last_kernel(offset, index_ref, state_ref, arrived_ref, head_ref, out_ref, rows_ref):
    count, width = out_ref.shape
    rows_ref[0:count, :] = state_ref[...]

    def body(step, carry):
        for u in range(16):
            t = step * 16 + u
            rows_ref[pl.ds(index_ref[offset + t], 1), :] = arrived_ref[pl.ds(t, 1), :]
        return carry

    lax.fori_loop(0, arrived_ref.shape[0] // 16, body, 0)
    lanes = lax.broadcasted_iota(jnp.int32, (128, width), 1)
    for b in range(count // 128):
        span = slice(b * 128, (b + 1) * 128)
        full = jnp.concatenate([head_ref[:, span], jnp.zeros((width - 8, 128), jnp.float32)], axis=0)
        out_ref[span, :] = jnp.where(lanes < 6, full.T, rows_ref[span, :])


def local(sizes, cap, state, velocity, cells, slots, counts):
    sections, _, cx, cy, depth = velocity.shape
    count, width = state.shape
    moving = 8 * cap
    fields = sections * 3
    field = velocity.reshape(fields, cx, cy, depth)
    rows = 2 * sections * moving // 128
    rows += -rows % 8
    edges = (4, fields + -fields % 8, depth)
    index, slot, taken, yface, away = pl.pallas_call(
        functools.partial(plan_kernel, cap),
        out_shape=(
            jax.ShapeDtypeStruct((rows, 128), jnp.int32),
            jax.ShapeDtypeStruct((sections, 1, moving), jnp.int32),
            jax.ShapeDtypeStruct((sections, 1, moving), jnp.float32),
            jax.ShapeDtypeStruct((2, fields, cx, depth), field.dtype),
            jax.ShapeDtypeStruct(edges, jnp.float32),
        ),
        in_specs=[VMEM, SMEM, VMEM],
        out_specs=(VMEM,) * 5,
    )(slots, counts.reshape(sections, 8), field.reshape(fields, cx * cy, depth))
    index = index.reshape(rows * 128)

    head, arrived = pl.pallas_call(
        functools.partial(steps_kernel, sizes, cap),
        out_shape=(
            jax.ShapeDtypeStruct((8, count), jnp.float32),
            jax.ShapeDtypeStruct((sections * moving, width), jnp.float32),
        ),
        in_specs=[SMEM] + [VMEM] * 7,
        out_specs=(VMEM, VMEM),
        scratch_shapes=[
            pltpu.VMEM((count + (sections - 1) * moving, width), jnp.float32),
            pltpu.VMEM((sections, moving, width), jnp.float32),
            pltpu.VMEM((2, count, moving), jnp.bfloat16),
            pltpu.VMEM((3 * depth, cx * cy + 2 * cx + 2 * cy + 16), jnp.bfloat16),
            pltpu.VMEM((fields, 2 * cx + 2 * cy, depth), jnp.bfloat16),
            pltpu.VMEM(edges, jnp.float32),
            pltpu.VMEM((sections, 8, 8, cap), jnp.float32),
            pltpu.VMEM((sections, 8, 8, cap), jnp.float32),
            pltpu.SemaphoreType.DMA((3 * sections, 8)),
            pltpu.SemaphoreType.DMA((3 * sections, 8)),
        ],
        compiler_params=pltpu.CompilerParams(collective_id=0, has_side_effects=True),
    )(
        index,
        slot,
        taken,
        cells,
        field,
        yface,
        away,
        state,
    )
    return pl.pallas_call(
        functools.partial(last_kernel, sections * moving),
        out_shape=jax.ShapeDtypeStruct((count, width), jnp.float32),
        in_specs=[SMEM, VMEM, VMEM, VMEM],
        out_specs=VMEM,
        scratch_shapes=[pltpu.VMEM((count + SPARE, width), jnp.float32)],
    )(index, state, arrived, head)


def solution(mesh):
    return jax.shard_map(
        functools.partial(local, (mesh.shape["gx"], mesh.shape["gy"]), 64),
        mesh=mesh,
        in_specs=(
            P(("gx", "gy"), None),
            P(None, None, "gx", "gy", None),
            P(None, None, ("gx", "gy")),
            P(None, ("gx", "gy")),
            P(None, "gx", "gy", None),
        ),
        out_specs=P(("gx", "gy"), None),
        check_vma=False,
    )
```

```python
import functools

import jax
import jax.numpy as jnp
from jax import lax
from jax.experimental import pallas as pl
from jax.experimental.pallas import tpu as pltpu
from jax.sharding import PartitionSpec as P

GAMMA = (8.0 / 15.0, 5.0 / 12.0, 3.0 / 4.0)
ZETA = (0.0, -17.0 / 60.0, -5.0 / 12.0)
OFFSETS = ((1, 0), (-1, 0), (0, 1), (0, -1), (1, 1), (-1, -1), (1, -1), (-1, 1))
SPARE = 8
BLOCK = 512
MESH = pl.DeviceIdType.MESH
VMEM = pl.BlockSpec(memory_space=pltpu.VMEM)
SMEM = pl.BlockSpec(memory_space=pltpu.SMEM)


def neighbour(r, sizes):
    off_x, off_y = OFFSETS[r]
    i, j = lax.axis_index("gx"), lax.axis_index("gy")
    return (lax.rem(i + off_x + sizes[0], sizes[0]), lax.rem(j + off_y + sizes[1], sizes[1]))


def greet(sizes):
    barrier = pltpu.get_barrier_semaphore()
    for r in range(8):
        pl.semaphore_signal(barrier, inc=1, device_id=neighbour(r, sizes), device_id_type=MESH)
    pl.semaphore_wait(barrier, 8)


def send(r, src, dst, sems, group, sizes):
    copy = pltpu.make_async_remote_copy(
        src_ref=src,
        dst_ref=dst,
        send_sem=sems[0].at[group, r],
        recv_sem=sems[1].at[group, r ^ 1],
        device_id=neighbour(r, sizes),
        device_id_type=MESH,
    )
    copy.start()
    return copy


def parts_of(x):
    high = x.astype(jnp.bfloat16)
    rest = x - high.astype(jnp.float32)
    middle = rest.astype(jnp.bfloat16)
    low = (rest - middle.astype(jnp.float32)).astype(jnp.bfloat16)
    return high, middle, low


def cell_weights(size, cell, frac):
    spots = lax.broadcasted_iota(jnp.int32, (size, cell.shape[1]), 0)
    low, high = 1.0 - frac, frac
    inside = jnp.where(spots == cell, low, 0.0) + jnp.where(spots == cell + 1, high, 0.0)
    return inside, jnp.where(cell == -1, low, 0.0), jnp.where(cell == size - 1, high, 0.0)


def gather_rows(order_ref, section, source_ref, leave_ref, cap):
    first = section * 8 * cap

    def body(step, carry):
        for u in range(16):
            t = step * 16 + u
            leave_ref[section, pl.ds(t, 1), :] = source_ref[pl.ds(order_ref[first + t], 1), :]
        return carry

    lax.fori_loop(0, 8 * cap // 16, body, 0)


def build_onehot(slot_ref, section, onehot_ref):
    slot = slot_ref[section]
    moving = slot.shape[1]
    step_rows = 256

    def body(step, carry):
        base = pl.multiple_of(step * step_rows, step_rows)
        spots = lax.broadcasted_iota(jnp.int32, (step_rows, moving), 0) + base
        onehot_ref[pl.ds(base, step_rows), :] = jnp.where(spots == slot, 1.0, 0.0).astype(jnp.bfloat16)
        return carry

    lax.fori_loop(0, onehot_ref.shape[0] // step_rows, body, 0)


def build_plane(section, dims, v_ref, halo_ref, corner_ref, plane_ref):
    cx, cy = dims
    inner = cx * cy
    depth = v_ref.shape[3]
    for k in range(3):
        row = 3 * section + k
        own = v_ref[row].reshape(inner, depth)
        plane_ref[pl.ds(k * depth, depth), 0:inner] = own.T
        faces = halo_ref[row].astype(jnp.float32)
        corners = [corner_ref[d, row : row + 1, :] for d in range(4)]
        filler = jnp.zeros((128 - faces.shape[0] - 4, depth), jnp.float32)
        edge = jnp.concatenate([faces] + corners + [filler], axis=0)
        width = plane_ref.shape[1] - inner
        plane_ref[pl.ds(k * depth, depth), inner:] = edge.T[:, 0:width].astype(jnp.bfloat16)


def sample(section, dims, head, cell, plane_ref):
    cx, cy = dims
    depth = plane_ref.shape[0] // 3
    block = head.shape[1]
    wx, wx_low, wx_high = cell_weights(cx, cell[0:1], head[0:1])
    wy, wy_low, wy_high = cell_weights(cy, cell[1:2], head[1:2])
    wz, _, _ = cell_weights(depth, cell[2:3], head[2:3])
    parts = [wx[x : x + 1] * wy for x in range(cx)]
    parts += [wx_high * wy, wx_low * wy, wx * wy_high, wx * wy_low]
    parts += [wx_high * wy_high, wx_low * wy_low, wx_high * wy_low, wx_low * wy_high]
    parts += [jnp.zeros((12, block), jnp.float32)]
    whole = jnp.concatenate(parts, axis=0)
    high = whole.astype(jnp.bfloat16)
    low = (whole - high.astype(jnp.float32)).astype(jnp.bfloat16)
    columns = jnp.dot(plane_ref[...], high, preferred_element_type=jnp.float32)
    columns = columns + jnp.dot(plane_ref[...], low, preferred_element_type=jnp.float32)
    speed = jnp.concatenate(
        [jnp.sum(columns[k * depth : (k + 1) * depth] * wz, axis=0, keepdims=True) for k in range(3)],
        axis=0,
    )
    moved = head[0:3] + GAMMA[section] * speed + ZETA[section] * head[3:6]
    return jnp.concatenate([moved, speed, jnp.ones((2, block), jnp.float32)], axis=0)


def sample_all(section, dims, cells_ref, head_ref, plane_ref):
    block = BLOCK

    def body(step, carry):
        span = pl.ds(pl.multiple_of(step * block, block), block)
        head_ref[:, span] = sample(section, dims, head_ref[:, span], cells_ref[section, :, span], plane_ref)
        return carry

    lax.fori_loop(0, head_ref.shape[1] // block, body, 0)


def plan_kernel(cap, slots_ref, counts_ref, v_ref, index_ref, slot_ref, taken_ref, yface_ref, away_ref):
    sections, count = slots_ref.shape
    moving = 8 * cap
    fields, inner, depth = v_ref.shape
    cx = yface_ref.shape[2]
    cy = inner // cx
    lanes = lax.broadcasted_iota(jnp.int32, (1, moving), 1)
    within = lax.rem(lanes, cap)
    places = lax.broadcasted_iota(jnp.int32, (moving, moving), 0) + count
    chunks = moving // 128
    columns = []
    for section in range(sections):
        slot = slots_ref[section : section + 1, 0:moving]
        limit = jnp.zeros((1, moving), jnp.int32)
        for r in range(8):
            limit = jnp.where(lanes >= r * cap, counts_ref[section, 0, 0, r], limit)
        taken = within < limit
        goal = jnp.where(taken, slot, count)
        found = jnp.full((1, moving), -1, jnp.int32)
        for past in range(section):
            match = columns[past] == slot
            best = jnp.max(jnp.where(match, places, -1), axis=0, keepdims=True)
            found = jnp.where(best >= 0, best + past * moving, found)
        source = jnp.where(found >= 0, found, slot)
        if section + 1 < sections:
            wide = jnp.broadcast_to(goal.astype(jnp.float32), (8, moving))
            columns.append(wide.T[:, 0:1].astype(jnp.int32))
        slot_ref[section] = slot
        taken_ref[section] = jnp.where(taken, 1.0, 0.0)
        for c in range(chunks):
            span = slice(c * 128, (c + 1) * 128)
            row = section * chunks + c
            index_ref[row : row + 1, :] = source[:, span]
            row += sections * chunks
            index_ref[row : row + 1, :] = goal[:, span]
    row = lax.broadcasted_iota(jnp.int32, (2 * cx + 8, inner), 0)
    place = lax.broadcasted_iota(jnp.int32, (2 * cx + 8, inner), 1)
    want = jnp.where(row < cx, row * cy + cy - 1, (row - cx) * cy)
    for d, spot in enumerate((inner - 1, 0, (cx - 1) * cy, cy - 1)):
        want = jnp.where(row == 2 * cx + d, spot, want)
    pick = jnp.where(want == place, 1.0, 0.0).astype(jnp.bfloat16)
    for f in range(fields):
        edge = jnp.dot(pick, v_ref[f], preferred_element_type=jnp.float32)
        yface_ref[0, f] = edge[0:cx].astype(jnp.bfloat16)
        yface_ref[1, f] = edge[cx : 2 * cx].astype(jnp.bfloat16)
        for d in range(4):
            away_ref[d, f : f + 1, :] = edge[2 * cx + d : 2 * cx + d + 1]


def steps_kernel(
    sizes,
    cap,
    order_ref,
    slot_ref,
    taken_ref,
    cells_ref,
    v_ref,
    yface_ref,
    away_ref,
    state_ref,
    head_ref,
    arrived_ref,
    rows_ref,
    leave_ref,
    onehot_ref,
    plane_ref,
    halo_ref,
    corner_ref,
    head_out_ref,
    head_in_ref,
    send_sem,
    recv_sem,
):
    sems = (send_sem, recv_sem)
    sections = slot_ref.shape[0]
    cx, cy = v_ref.shape[1], v_ref.shape[2]
    count = state_ref.shape[0]
    moving = 8 * cap
    starts = (0, cy, 2 * cy, 2 * cy + cx)
    widths = (cy, cy, cx, cx)
    greet(sizes)

    halos = []
    for section in range(sections):
        group = []
        fields = pl.ds(3 * section, 3)
        for r in range(4):
            off_x, off_y = OFFSETS[r]
            src = v_ref.at[fields, cx - 1 if off_x > 0 else 0] if off_x else yface_ref.at[r - 2, fields]
            dst = halo_ref.at[fields, pl.ds(starts[r ^ 1], widths[r ^ 1]), :]
            group.append(send(r, src, dst, sems, section, sizes))
        if section == 0:
            for r in range(4, 8):
                group.append(send(r, away_ref.at[r - 4], corner_ref.at[(r ^ 1) - 4], sems, section, sizes))
        halos.append(group)

    def send_rows(section):
        gather_rows(order_ref, section, rows_ref, leave_ref, cap)
        return [
            send(
                r,
                leave_ref.at[section, pl.ds(r * cap, cap)],
                arrived_ref.at[pl.ds(section * moving + (r ^ 1) * cap, cap)],
                sems,
                sections + section,
                sizes,
            )
            for r in range(8)
        ]

    rows_ref[0:count, :] = state_ref[...]
    carried = send_rows(0)
    for b in range(count // 128):
        head_ref[:, b * 128 : (b + 1) * 128] = state_ref[b * 128 : (b + 1) * 128, :].T[0:8]
    for section in range(sections):
        if section == 0:
            build_onehot(slot_ref, 0, onehot_ref.at[0])
        hot = onehot_ref.at[section % 2]
        where_ = cells_ref[section].astype(jnp.float32)
        stacked = [part.astype(jnp.float32) for part in parts_of(head_ref[...])] + [where_]
        stacked = jnp.concatenate(stacked, axis=0).astype(jnp.bfloat16)
        picked = jnp.dot(stacked, hot[...], preferred_element_type=jnp.float32)
        leaving = picked[0:8] + picked[8:16] + picked[16:24]
        there = picked[24:27].astype(jnp.int32)
        for copy in halos[section]:
            copy.wait()
        build_plane(section, (cx, cy), v_ref, halo_ref, corner_ref, plane_ref)
        leaving = jnp.concatenate(
            [
                sample(section, (cx, cy), leaving[:, b : b + BLOCK], there[:, b : b + BLOCK], plane_ref)
                for b in range(0, moving, BLOCK)
            ],
            axis=1,
        )
        heads = []
        for r in range(8):
            head_out_ref[section, r] = leaving[:, r * cap : (r + 1) * cap]
        for r in range(8):
            heads.append(
                send(
                    r,
                    head_out_ref.at[section, r],
                    head_in_ref.at[section, r ^ 1],
                    sems,
                    2 * sections + section,
                    sizes,
                )
            )
        sample_all(section, (cx, cy), cells_ref, head_ref, plane_ref)
        for copy in carried:
            copy.wait()
        if section + 1 < sections:
            low = section * moving
            rows_ref[count + low : count + low + moving, :] = arrived_ref[low : low + moving, :]
            carried = send_rows(section + 1)
            build_onehot(slot_ref, section + 1, onehot_ref.at[(section + 1) % 2])
        for copy in heads:
            copy.wait()
        came = jnp.concatenate([head_in_ref[section, r] for r in range(8)], axis=1)
        came = came * taken_ref[section]
        stacked = jnp.concatenate([part.astype(jnp.float32) for part in parts_of(came)], axis=0)
        spread = lax.dot_general(
            stacked.astype(jnp.bfloat16), hot[...], (((1,), (1,)), ((), ())), preferred_element_type=jnp.float32
        )
        placed = spread[0:8] + spread[8:16] + spread[16:24]
        head_ref[...] = jnp.where(placed[6:7] > 0.5, placed, head_ref[...])


def last_kernel(offset, index_ref, state_ref, arrived_ref, head_ref, out_ref, rows_ref):
    count, width = out_ref.shape
    rows_ref[0:count, :] = state_ref[...]

    def body(step, carry):
        for u in range(16):
            t = step * 16 + u
            rows_ref[pl.ds(index_ref[offset + t], 1), :] = arrived_ref[pl.ds(t, 1), :]
        return carry

    lax.fori_loop(0, arrived_ref.shape[0] // 16, body, 0)
    lanes = lax.broadcasted_iota(jnp.int32, (128, width), 1)
    for b in range(count // 128):
        span = slice(b * 128, (b + 1) * 128)
        full = jnp.concatenate([head_ref[:, span], jnp.zeros((width - 8, 128), jnp.float32)], axis=0)
        out_ref[span, :] = jnp.where(lanes < 6, full.T, rows_ref[span, :])


def local(sizes, cap, state, velocity, cells, slots, counts):
    sections, _, cx, cy, depth = velocity.shape
    count, width = state.shape
    moving = 8 * cap
    fields = sections * 3
    field = velocity.reshape(fields, cx, cy, depth)
    rows = 2 * sections * moving // 128
    rows += -rows % 8
    edges = (4, fields + -fields % 8, depth)
    index, slot, taken, yface, away = pl.pallas_call(
        functools.partial(plan_kernel, cap),
        out_shape=(
            jax.ShapeDtypeStruct((rows, 128), jnp.int32),
            jax.ShapeDtypeStruct((sections, 1, moving), jnp.int32),
            jax.ShapeDtypeStruct((sections, 1, moving), jnp.float32),
            jax.ShapeDtypeStruct((2, fields, cx, depth), field.dtype),
            jax.ShapeDtypeStruct(edges, jnp.float32),
        ),
        in_specs=[VMEM, SMEM, VMEM],
        out_specs=(VMEM,) * 5,
    )(slots, counts, field.reshape(fields, cx * cy, depth))
    index = index.reshape(rows * 128)

    head, arrived = pl.pallas_call(
        functools.partial(steps_kernel, sizes, cap),
        out_shape=(
            jax.ShapeDtypeStruct((8, count), jnp.float32),
            jax.ShapeDtypeStruct((sections * moving, width), jnp.float32),
        ),
        in_specs=[SMEM] + [VMEM] * 7,
        out_specs=(VMEM, VMEM),
        scratch_shapes=[
            pltpu.VMEM((count + (sections - 1) * moving, width), jnp.float32),
            pltpu.VMEM((sections, moving, width), jnp.float32),
            pltpu.VMEM((2, count, moving), jnp.bfloat16),
            pltpu.VMEM((3 * depth, cx * cy + 2 * cx + 2 * cy + 16), jnp.bfloat16),
            pltpu.VMEM((fields, 2 * cx + 2 * cy, depth), jnp.bfloat16),
            pltpu.VMEM(edges, jnp.float32),
            pltpu.VMEM((sections, 8, 8, cap), jnp.float32),
            pltpu.VMEM((sections, 8, 8, cap), jnp.float32),
            pltpu.SemaphoreType.DMA((3 * sections, 8)),
            pltpu.SemaphoreType.DMA((3 * sections, 8)),
        ],
        compiler_params=pltpu.CompilerParams(collective_id=0, has_side_effects=True),
    )(
        index,
        slot,
        taken,
        cells,
        field,
        yface,
        away,
        state,
    )
    return pl.pallas_call(
        functools.partial(last_kernel, sections * moving),
        out_shape=jax.ShapeDtypeStruct((count, width), jnp.float32),
        in_specs=[SMEM, VMEM, VMEM, VMEM],
        out_specs=VMEM,
        scratch_shapes=[pltpu.VMEM((count + SPARE, width), jnp.float32)],
    )(index, state, arrived, head)


def solution(mesh):
    return jax.shard_map(
        functools.partial(local, (mesh.shape["gx"], mesh.shape["gy"]), 64),
        mesh=mesh,
        in_specs=(
            P(("gx", "gy"), None),
            P(None, None, "gx", "gy", None),
            P(None, None, ("gx", "gy")),
            P(None, ("gx", "gy")),
            P(None, "gx", "gy", None),
        ),
        out_specs=P(("gx", "gy"), None),
        check_vma=False,
    )
```
